512 devices in a mesh: orb: 512 (over z, y, x, core).
Axes of the slice: x: 4, y: 4, z: 16, core: 2. Of those that a mesh axis runs over, the one named last changes fastest.
Arguments:
- orbitals: bfloat16 [512, 48, 2304], P('orb'), may hold values from -6 to 6
- pair_mask: int32 [2, 512], replicated, may hold values from 0 to 1, as said below
- offsets: int32 [3, 2, 512], replicated, may hold values from -12 to 12
Outputs:
- exchange: bfloat16 [512, 48, 2304], P('orb')
The draws below stay inside these ranges and needn't reach their ends.
Inputs may be any that keep to these rules, and one draw needn't show every extreme that they name: `pair_mask`: in every matching, the pair that holds orbital 0 and the pair that holds orbital 512 - 1 are live.
All inputs are finite; a program needn't handle non-finite values.
Results may differ from the reference program's by a relative error of at most 0.004.
Values may be sent and summed in bfloat16 or wider, within the bound.
No kernel may reach another device: no remote copies, remote signals or barrier semaphores. Data moves between devices by JAX's collectives and lax.ppermute only.
A program may use at most 64 MiB of HBM per device.

```python
import math
import jax
import jax.numpy as jnp
import numpy as np
from jax import lax

BOX = 48
MATCH = 2
ORBITALS = 512
OMAX = 12
N_ORB = 512


def draw_pair_mask(key, part):
    mixed = jax.random.fold_in(key, 7301)
    values = jax.random.randint(mixed, (MATCH, ORBITALS), 0, 4, dtype=jnp.int32)
    live = jnp.where(values < 3, 1, 0).astype(jnp.int32)
    levels = ORBITALS.bit_length() - 1
    places = jnp.arange(ORBITALS, dtype=jnp.int32)
    rows = []
    for match_index in range(MATCH):
        bit_pos = match_index * (levels - 1) // (MATCH - 1)
        top_lower = ORBITALS - 1 - (1 << bit_pos)
        forced = (places == 0) | (places == top_lower)
        rows.append(jnp.where(forced, 1, live[match_index]).astype(jnp.int32))
    return jnp.stack(rows, axis=0)


def touch_ends(result, stream_key, low, high):
    shape = result.shape
    index_at = [jax.random.randint(jax.random.fold_in(stream_key, axis), (), 0, shape[axis]) for axis in range(len(shape))]
    result = result.at[tuple(index_at)].set(low)
    longest = shape.index(max(shape))
    index_at[longest] = (index_at[longest] + 1) % shape[longest]
    return result.at[tuple(index_at)].set(high)


def block_scale(rng, shape, cuts, low, high):
    level = 1.0
    for axis_at, shards_of in cuts:
        heights = jax.random.uniform(jax.random.fold_in(jax.random.fold_in(rng, 6), axis_at), (shards_of,), jnp.float32, low / len(cuts), high / len(cuts))
        level = level * jnp.repeat(jnp.exp(heights), shape[axis_at] // shards_of).reshape((-1,) + (1,) * (len(shape) - 1 - axis_at))
    return level


def scatter_about(own_key, shape, deviation, most, split=(), kind=jnp.bfloat16):
    level = block_scale(own_key, shape, split, -0.22, 0.18) if split else 1.0
    values = jax.random.normal(own_key, shape, jnp.float32) * deviation * level
    return jnp.minimum(jnp.maximum(values, -most), most).astype(kind)


def setup_inputs(seed: int = 0) -> dict:
    arg_keys = jax.random.split(jax.random.key(seed), 4)
    return {
        "orbitals": scatter_about(arg_keys[0], (ORBITALS, BOX, BOX * BOX), 1.0, 6.0, ((0, 512),)),
        "pair_mask": draw_pair_mask(jax.random.fold_in(arg_keys[3], 71), 0),
        "offsets": touch_ends(jax.random.randint(arg_keys[2], (3, MATCH, ORBITALS), -OMAX, OMAX + 1), jax.random.fold_in(arg_keys[2], 1), -OMAX, OMAX).astype(jnp.int32),
    }


screening = 0.5

def sine_table(extent):
    modes = jnp.arange(1, extent + 1, dtype=jnp.int32).astype(jnp.float32)
    angles = math.pi * modes[:, None] * modes[None, :] / (extent + 1)
    return math.sqrt(2.0 / (extent + 1)) * jnp.sin(angles)

def inverse_symbol(extent):
    modes = jnp.arange(1, extent + 1, dtype=jnp.int32).astype(jnp.float32)
    eigenvalue = 2.0 - 2.0 * jnp.cos(math.pi * modes / (extent + 1))
    summed_eigen = eigenvalue[:, None, None] + eigenvalue[None, :, None] + eigenvalue[None, None, :]
    return 1.0 / (summed_eigen + screening)

def transform(volume, sines):
    exact = lax.Precision.HIGHEST
    volume = jnp.einsum('ai,ijk->ajk', sines, volume, precision=exact)
    volume = jnp.einsum('bj,ajk->abk', sines, volume, precision=exact)
    return jnp.einsum('ck,abk->abc', sines, volume, precision=exact)

def shift_box(volume, offset):
    extent = volume.shape[0]
    places = jnp.arange(extent, dtype=jnp.int32)
    for axis_pos in range(3):
        volume = jnp.roll(volume, offset[axis_pos], axis=axis_pos)
        source = places - offset[axis_pos]
        inside = (source >= 0) & (source < extent)
        view_shape = [1, 1, 1]
        view_shape[axis_pos] = extent
        volume = jnp.where(inside.reshape(view_shape), volume, jnp.zeros_like(volume))
    return volume

def pair_terms(phi_low, phi_up, offset, sines, symbol):
    visitor = shift_box(phi_up, offset)
    density = phi_low * visitor
    potential = transform(symbol * transform(density, sines), sines)
    lower_term = (potential * visitor).astype(jnp.bfloat16)
    upper_term = shift_box(potential * phi_low, -offset).astype(jnp.bfloat16)
    return (lower_term, upper_term)

def reference(orbitals, pair_mask, offsets):
    volumes = orbitals.reshape(ORBITALS, BOX, BOX, BOX)
    sines = sine_table(BOX)
    symbol = inverse_symbol(BOX)
    levels = N_ORB.bit_length() - 1
    everyone = np.arange(ORBITALS)
    summed = jnp.zeros((ORBITALS, BOX, BOX, BOX), jnp.float32)
    for match_index in range(MATCH):
        bit_pos = match_index * (levels - 1) // (MATCH - 1)
        lowers = everyone[(everyone >> bit_pos) % 2 == 0]
        uppers = lowers + (1 << bit_pos)

        def one_pair(items):
            low_orb, up_orb, offset, live = items
            lower_term, upper_term = pair_terms(low_orb.astype(jnp.float32), up_orb.astype(jnp.float32), offset, sines, symbol)
            lower_term = jnp.where(live > 0, lower_term, jnp.zeros_like(lower_term))
            upper_term = jnp.where(live > 0, upper_term, jnp.zeros_like(upper_term))
            return (lower_term, upper_term)
        pair_offsets = jnp.transpose(offsets[:, match_index, lowers]).astype(jnp.int32)
        lower_all, upper_all = lax.map(one_pair, (volumes[lowers], volumes[uppers], pair_offsets, pair_mask[match_index, lowers]))
        summed = summed.at[lowers].add(lower_all.astype(jnp.float32))
        summed = summed.at[uppers].add(upper_all.astype(jnp.float32))
    return (-summed).astype(jnp.bfloat16).reshape(ORBITALS, BOX, BOX * BOX)
```

```python
import jax
import jax.numpy as jnp
import numpy as np
from jax import lax
from jax.experimental import pallas as pl
from jax.experimental.pallas import tpu as pltpu
from jax.sharding import PartitionSpec as P

SCREENING = 0.5
BOX = 48
WIDE = 64
LANES = 128
FLAT = BOX * BOX
TILES = FLAT // LANES
GROUPS = 6
PAIRS = BOX // 2
EDGE = 5
ROWPAD = 16
ROWS = BOX + 2 * ROWPAD

F32 = jnp.float32
BF16 = jnp.bfloat16


def split_np(table):
    high = table.astype(np.float32).astype(jnp.bfloat16)
    low = (table - high.astype(np.float64)).astype(np.float32).astype(jnp.bfloat16)
    return high, low


def tables():
    modes = np.arange(1, BOX + 1, dtype=np.float64)
    sines = np.sqrt(2.0 / (BOX + 1)) * np.sin(np.pi * modes[:, None] * modes[None, :] / (BOX + 1))
    eigen = 2.0 - 2.0 * np.cos(np.pi * modes / (BOX + 1))

    def stacked(matrix):
        high, low = split_np(matrix)
        return np.concatenate([high, high, low], axis=1)

    order = np.concatenate([np.arange(0, BOX, 2), np.arange(1, BOX, 2)])
    over_a = stacked(sines)
    over_b = stacked(sines[:, order])
    back_b = stacked(sines[order, :])
    narrow = np.zeros((8 * BOX, 8 * WIDE))
    for row in range(8):
        narrow[row * BOX : (row + 1) * BOX, row * WIDE : row * WIDE + BOX] = sines
    fore_c = np.stack([narrow[0:256, 0:256], narrow[128:384, 256:512]])
    widened = narrow.T
    back_c = np.stack([widened[128 * n : 128 * n + 256, 128 * n : 128 * n + 128] for n in range(3)])
    symbol = np.zeros((BOX, BOX, WIDE))
    symbol[:, :, :BOX] = 1.0 / (
        eigen[:, None, None] + eigen[None, :, None] + eigen[None, None, :] + SCREENING
    )
    symbol = np.transpose(symbol, (1, 0, 2)).reshape(BOX, BOX * WIDE).astype(np.float32)
    fore_c = np.stack(split_np(fore_c))
    back_c = np.stack(split_np(back_c))
    return over_a, over_b, back_b, fore_c, back_c, symbol


def split(x):
    high = x.astype(BF16)
    low = (x - high.astype(F32)).astype(BF16)
    return high, low


def apply_rows(matrix, x):
    high, low = split(x)
    return jnp.dot(matrix, jnp.concatenate([high, low, high], axis=0), preferred_element_type=F32)


def apply_lanes(parts, table):
    splits = [split(x) for x in parts]
    highs = jnp.concatenate([h for h, _ in splits], axis=0)
    lows = jnp.concatenate([l for _, l in splits], axis=0)
    out = jnp.dot(highs, table[0], preferred_element_type=F32)
    out = out + jnp.dot(lows, table[0], preferred_element_type=F32)
    out = out + jnp.dot(highs, table[1], preferred_element_type=F32)
    return [out[BOX * i : BOX * (i + 1)] for i in range(len(parts))]


def make_kernel(match_index, bit_pos, last):
    def kernel(*refs):
        me_ref, mask_ref, off_ref, mine_ref, partner_ref = refs[:5]
        at = 5
        if last:
            prev_ref = refs[at]
            at += 1
        over_a_ref, over_b_ref, back_b_ref, fore_c_ref, back_c_ref, symbol_ref = refs[at : at + 6]
        out_ref, pad_ref, flip_ref = refs[at + 6 :]

        me = me_ref[0]
        upper_bit = (me >> bit_pos) & 1
        lower = me - (upper_bit << bit_pos)
        is_low = upper_bit == 0
        live = mask_ref[match_index, lower] > 0
        off = [off_ref[d, match_index, lower] for d in range(3)]

        lane = lax.broadcasted_iota(jnp.int32, (1, LANES), 1)

        def fill(tiles):
            for j in range(TILES):
                pad_ref[EDGE + j, ROWPAD : ROWPAD + BOX, :] = tiles[j]

        def shifted(o):
            start = EDGE * LANES - (o[1] * BOX + o[2])
            tile = start >> 7
            rest = start & (LANES - 1)
            turn = (LANES - rest) & (LANES - 1)
            keep = lane < LANES - rest
            rows = pl.ds(ROWPAD - o[0], BOX)
            rolled = [pltpu.roll(pad_ref[tile + j, rows, :], turn, axis=1) for j in range(TILES + 1)]
            result = []
            for j in range(TILES):
                flat = lane + LANES * j
                place = flat - ((flat * 43691) >> 21) * BOX - o[2]
                inside = jnp.where((place >= 0) & (place < BOX), 1.0, 0.0).astype(F32)
                here = jnp.where(keep, inside, 0.0)
                there = inside - here
                result.append(rolled[j] * here + rolled[j + 1] * there)
            return result

        def tile_of(ref, j):
            return ref[0, :, LANES * j : LANES * (j + 1)].astype(F32)

        def emit(j, term):
            cols = slice(LANES * j, LANES * (j + 1))
            if last:
                out_ref[0, :, cols] = (-(prev_ref[0, :, cols].astype(F32) + term)).astype(BF16)
            else:
                out_ref[0, :, cols] = term.astype(BF16)

        @pl.when(live)
        def _():
            zero_rows = jnp.zeros((ROWS, LANES), F32)
            for j in range(2 * EDGE + TILES):
                pad_ref[j] = zero_rows
            low_f = jnp.where(is_low, 1.0, 0.0).astype(F32)
            low_v = jnp.full((1, LANES), low_f, F32) > 0.5
            mine = [tile_of(mine_ref, j) for j in range(TILES)]
            partner = [tile_of(partner_ref, j) for j in range(TILES)]
            fill([jnp.where(low_v, p, m) for p, m in zip(partner, mine)])
            visitor = shifted(off)
            other = [jnp.where(low_v, m, p) for p, m in zip(partner, mine)]
            density = [o * v for o, v in zip(other, visitor)]
            factor = [jnp.where(low_v, v, o) for o, v in zip(other, visitor)]

            over_a = over_a_ref[...]
            wide = [
                apply_rows(over_a, jnp.concatenate(density[3 * g : 3 * g + 3], axis=1))
                for g in range(GROUPS)
            ]
            for h in range(2):
                got = apply_lanes(
                    [w[:, LANES * h : LANES * h + 256] for w in wide], (fore_c_ref[0, h], fore_c_ref[1, h])
                )
                for g in range(GROUPS):
                    for k in range(2):
                        row = (4 * g + 2 * h + k) * BOX
                        flip_ref[row : row + BOX, :] = got[g][:, LANES * k : LANES * (k + 1)]

            over_b = over_b_ref[...]
            back_b = back_b_ref[...]
            first = lane < WIDE
            backs = []
            for pair in range(PAIRS // 2):
                cols = []
                for u in (2 * pair, 2 * pair + 1):
                    even = flip_ref[pl.ds(2 * u, PAIRS, stride=BOX), :]
                    odd = flip_ref[pl.ds(2 * u + 1, PAIRS, stride=BOX), :]
                    upper = jnp.where(first, even, pltpu.roll(odd, WIDE, axis=1))
                    under = jnp.where(first, pltpu.roll(even, WIDE, axis=1), odd)
                    cols.append(jnp.concatenate([upper, under], axis=0))
                modes = apply_rows(over_b, jnp.concatenate(cols, axis=1))
                modes = modes * symbol_ref[:, 256 * pair : 256 * (pair + 1)]
                backs.append(apply_rows(back_b, modes))
            for pair in range(PAIRS // 2):
                for k in range(2):
                    u = 2 * pair + k
                    block = backs[pair][:, LANES * k : LANES * (k + 1)]
                    upper, under = block[:PAIRS], block[PAIRS:]
                    even = jnp.where(first, upper, pltpu.roll(under, WIDE, axis=1))
                    odd = jnp.where(first, pltpu.roll(upper, WIDE, axis=1), under)
                    flip_ref[pl.ds(2 * u, PAIRS, stride=BOX), :] = even
                    flip_ref[pl.ds(2 * u + 1, PAIRS, stride=BOX), :] = odd

            narrow = [[None] * 3 for _ in range(GROUPS)]
            for n in range(3):
                parts = []
                for g in range(GROUPS):
                    row = (4 * g + n) * BOX
                    parts.append(
                        jnp.concatenate(
                            [flip_ref[row : row + BOX, :], flip_ref[row + BOX : row + 2 * BOX, :]], axis=1
                        )
                    )
                got = apply_lanes(parts, (back_c_ref[0, n], back_c_ref[1, n]))
                for g in range(GROUPS):
                    narrow[g][n] = got[g]
            product = []
            for g in range(GROUPS):
                potential = apply_rows(over_a, jnp.concatenate(narrow[g], axis=1))
                for n in range(3):
                    product.append(potential[:, LANES * n : LANES * (n + 1)] * factor[3 * g + n])
            fill([p.astype(BF16).astype(F32) for p in product])
            term = shifted([jnp.where(is_low, 0, -o) for o in off])
            for j in range(TILES):
                emit(j, term[j])

        @pl.when(jnp.logical_not(live))
        def _():
            nothing = jnp.zeros((BOX, LANES), F32)
            for j in range(TILES):
                emit(j, nothing)

    return kernel


def pair_call(match_index, bit_pos, last, me, pair_mask, offsets, mine, partner, prev, consts):
    smem = pl.BlockSpec(memory_space=pltpu.SMEM)
    vmem = pl.BlockSpec(memory_space=pltpu.VMEM)
    operands = [me, pair_mask, offsets, mine, partner] + ([prev] if last else []) + list(consts)
    specs = [smem] * 3 + [vmem] * (len(operands) - 3)
    return pl.pallas_call(
        make_kernel(match_index, bit_pos, last),
        out_shape=jax.ShapeDtypeStruct(mine.shape, BF16),
        in_specs=specs,
        out_specs=vmem,
        scratch_shapes=[
            pltpu.VMEM((2 * EDGE + TILES, ROWS, LANES), F32),
            pltpu.VMEM((PAIRS * BOX, LANES), F32),
        ],
        name="pair_last" if last else "pair_first",
    )(*operands)


def from_partner(block, axis, stride):
    count = lax.axis_size(axis)
    route = []
    for low in range(count):
        high = low | 1 << stride
        if high != low and high < count:
            route += [(low, high), (high, low)]
    return lax.ppermute(block, axis, route)


def per_device(orbitals, pair_mask, offsets):
    devices = lax.axis_size("orb")
    levels = devices.bit_length() - 1
    me = lax.axis_index("orb").astype(jnp.int32).reshape(1)
    matches = pair_mask.shape[0]
    consts = [jnp.asarray(t) for t in tables()]
    bits = [m * (levels - 1) // (matches - 1) for m in range(matches)]
    partners = [from_partner(orbitals, "orb", bit) for bit in bits]
    near = pair_call(0, bits[0], False, me, pair_mask, offsets, orbitals, partners[0], None, consts)
    return pair_call(1, bits[1], True, me, pair_mask, offsets, orbitals, partners[1], near, consts)


def solution(mesh):
    placed = (P("orb", None, None), P(), P())
    return jax.shard_map(
        per_device, mesh=mesh, in_specs=placed, out_specs=P("orb", None, None), check_vma=False
    )
```

```python
import jax
import jax.numpy as jnp
import numpy as np
from jax import lax
from jax.experimental import pallas as pl
from jax.experimental.pallas import tpu as pltpu
from jax.sharding import PartitionSpec as P


SCREENING = 0.5
BOX = 48
WIDE = 64
LANES = 128
FLAT = BOX * BOX
TILES = FLAT // LANES
GROUPS = 6
PAIRS = BOX // 2
EDGE = 5
ROWPAD = 16
ROWS = BOX + 2 * ROWPAD

F32 = jnp.float32
BF16 = jnp.bfloat16


def split_np(table):
    high = table.astype(np.float32).astype(jnp.bfloat16)
    low = (table - high.astype(np.float64)).astype(np.float32).astype(jnp.bfloat16)
    return high, low


def tables():
    modes = np.arange(1, BOX + 1, dtype=np.float64)
    sines = np.sqrt(2.0 / (BOX + 1)) * np.sin(np.pi * modes[:, None] * modes[None, :] / (BOX + 1))
    eigen = 2.0 - 2.0 * np.cos(np.pi * modes / (BOX + 1))

    def stacked(matrix):
        high, low = split_np(matrix)
        return np.concatenate([high, high, low], axis=1)

    order = np.concatenate([np.arange(0, BOX, 2), np.arange(1, BOX, 2)])
    over_a = stacked(sines)
    over_b = stacked(sines[:, order])
    back_b = stacked(sines[order, :])
    narrow = np.zeros((8 * BOX, 8 * WIDE))
    for row in range(8):
        narrow[row * BOX : (row + 1) * BOX, row * WIDE : row * WIDE + BOX] = sines
    fore_c = np.stack([narrow[0:256, 0:256], narrow[128:384, 256:512]])
    widened = narrow.T
    back_c = np.stack([widened[128 * n : 128 * n + 256, 128 * n : 128 * n + 128] for n in range(3)])
    symbol = np.zeros((BOX, BOX, WIDE))
    symbol[:, :, :BOX] = 1.0 / (
        eigen[:, None, None] + eigen[None, :, None] + eigen[None, None, :] + SCREENING
    )
    symbol = np.transpose(symbol, (1, 0, 2)).reshape(BOX, BOX * WIDE).astype(np.float32)
    fore_c = np.stack(split_np(fore_c))
    back_c = np.stack(split_np(back_c))
    return over_a, over_b, back_b, fore_c, back_c, symbol


def split(x):
    high = x.astype(BF16)
    low = (x - high.astype(F32)).astype(BF16)
    return high, low


def apply_rows(matrix, x):
    high, low = split(x)
    return jnp.dot(matrix, jnp.concatenate([high, low, high], axis=0), preferred_element_type=F32)


def apply_lanes(parts, table):
    splits = [split(x) for x in parts]
    highs = jnp.concatenate([h for h, _ in splits], axis=0)
    lows = jnp.concatenate([l for _, l in splits], axis=0)
    out = jnp.dot(highs, table[0], preferred_element_type=F32)
    out = out + jnp.dot(lows, table[0], preferred_element_type=F32)
    out = out + jnp.dot(highs, table[1], preferred_element_type=F32)
    return [out[BOX * i : BOX * (i + 1)] for i in range(len(parts))]


def make_kernel(match_index, bit_pos, last):
    def kernel(*refs):
        me_ref, mask_ref, off_ref, mine_ref, partner_ref = refs[:5]
        at = 5
        if last:
            prev_ref = refs[at]
            at += 1
        over_a_ref, over_b_ref, back_b_ref, fore_c_ref, back_c_ref, symbol_ref = refs[at : at + 6]
        out_ref, pad_ref, flip_ref = refs[at + 6 :]

        me = me_ref[0]
        upper_bit = (me >> bit_pos) & 1
        lower = me - (upper_bit << bit_pos)
        is_low = upper_bit == 0
        live = mask_ref[match_index, lower] > 0
        off = [off_ref[d, match_index, lower] for d in range(3)]

        lane = lax.broadcasted_iota(jnp.int32, (1, LANES), 1)

        def fill(tiles):
            for j in range(TILES):
                pad_ref[EDGE + j, ROWPAD : ROWPAD + BOX, :] = tiles[j]

        def shifted(o):
            start = EDGE * LANES - (o[1] * BOX + o[2])
            tile = start >> 7
            rest = start & (LANES - 1)
            turn = (LANES - rest) & (LANES - 1)
            keep = lane < LANES - rest
            rows = pl.ds(ROWPAD - o[0], BOX)
            rolled = [pltpu.roll(pad_ref[tile + j, rows, :], turn, axis=1) for j in range(TILES + 1)]
            result = []
            for j in range(TILES):
                flat = lane + LANES * j
                place = flat - ((flat * 43691) >> 21) * BOX - o[2]
                inside = jnp.where((place >= 0) & (place < BOX), 1.0, 0.0).astype(F32)
                here = jnp.where(keep, inside, 0.0)
                there = inside - here
                result.append(rolled[j] * here + rolled[j + 1] * there)
            return result

        def tile_of(ref, j):
            return ref[0, :, LANES * j : LANES * (j + 1)].astype(F32)

        def emit(j, term):
            cols = slice(LANES * j, LANES * (j + 1))
            if last:
                out_ref[0, :, cols] = (-(prev_ref[0, :, cols].astype(F32) + term)).astype(BF16)
            else:
                out_ref[0, :, cols] = term.astype(BF16)

        @pl.when(live)
        def _():
            zero_rows = jnp.zeros((ROWS, LANES), F32)
            for j in range(2 * EDGE + TILES):
                pad_ref[j] = zero_rows
            low_f = jnp.where(is_low, 1.0, 0.0).astype(F32)
            low_v = jnp.full((1, LANES), low_f, F32) > 0.5
            mine = [tile_of(mine_ref, j) for j in range(TILES)]
            partner = [tile_of(partner_ref, j) for j in range(TILES)]
            fill([jnp.where(low_v, p, m) for p, m in zip(partner, mine)])
            visitor = shifted(off)
            other = [jnp.where(low_v, m, p) for p, m in zip(partner, mine)]
            density = [o * v for o, v in zip(other, visitor)]
            factor = [jnp.where(low_v, v, o) for o, v in zip(other, visitor)]

            over_a = over_a_ref[...]
            wide = [
                apply_rows(over_a, jnp.concatenate(density[3 * g : 3 * g + 3], axis=1))
                for g in range(GROUPS)
            ]
            for h in range(2):
                got = apply_lanes(
                    [w[:, LANES * h : LANES * h + 256] for w in wide], (fore_c_ref[0, h], fore_c_ref[1, h])
                )
                for g in range(GROUPS):
                    for k in range(2):
                        row = (4 * g + 2 * h + k) * BOX
                        flip_ref[row : row + BOX, :] = got[g][:, LANES * k : LANES * (k + 1)]

            over_b = over_b_ref[...]
            back_b = back_b_ref[...]
            first = lane < WIDE
            backs = []
            for pair in range(PAIRS // 2):
                cols = []
                for u in (2 * pair, 2 * pair + 1):
                    even = flip_ref[pl.ds(2 * u, PAIRS, stride=BOX), :]
                    odd = flip_ref[pl.ds(2 * u + 1, PAIRS, stride=BOX), :]
                    upper = jnp.where(first, even, pltpu.roll(odd, WIDE, axis=1))
                    under = jnp.where(first, pltpu.roll(even, WIDE, axis=1), odd)
                    cols.append(jnp.concatenate([upper, under], axis=0))
                modes = apply_rows(over_b, jnp.concatenate(cols, axis=1))
                modes = modes * symbol_ref[:, 256 * pair : 256 * (pair + 1)]
                backs.append(apply_rows(back_b, modes))
            for pair in range(PAIRS // 2):
                for k in range(2):
                    u = 2 * pair + k
                    block = backs[pair][:, LANES * k : LANES * (k + 1)]
                    upper, under = block[:PAIRS], block[PAIRS:]
                    even = jnp.where(first, upper, pltpu.roll(under, WIDE, axis=1))
                    odd = jnp.where(first, pltpu.roll(upper, WIDE, axis=1), under)
                    flip_ref[pl.ds(2 * u, PAIRS, stride=BOX), :] = even
                    flip_ref[pl.ds(2 * u + 1, PAIRS, stride=BOX), :] = odd

            narrow = [[None] * 3 for _ in range(GROUPS)]
            for n in range(3):
                parts = []
                for g in range(GROUPS):
                    row = (4 * g + n) * BOX
                    parts.append(
                        jnp.concatenate(
                            [flip_ref[row : row + BOX, :], flip_ref[row + BOX : row + 2 * BOX, :]], axis=1
                        )
                    )
                got = apply_lanes(parts, (back_c_ref[0, n], back_c_ref[1, n]))
                for g in range(GROUPS):
                    narrow[g][n] = got[g]
            product = []
            for g in range(GROUPS):
                potential = apply_rows(over_a, jnp.concatenate(narrow[g], axis=1))
                for n in range(3):
                    product.append(potential[:, LANES * n : LANES * (n + 1)] * factor[3 * g + n])
            fill([p.astype(BF16).astype(F32) for p in product])
            term = shifted([jnp.where(is_low, 0, -o) for o in off])
            for j in range(TILES):
                emit(j, term[j])

        @pl.when(jnp.logical_not(live))
        def _():
            nothing = jnp.zeros((BOX, LANES), F32)
            for j in range(TILES):
                emit(j, nothing)

    return kernel


def pair_call(match_index, bit_pos, last, me, pair_mask, offsets, mine, partner, prev, consts):
    smem = pl.BlockSpec(memory_space=pltpu.SMEM)
    vmem = pl.BlockSpec(memory_space=pltpu.VMEM)
    operands = [me, pair_mask, offsets, mine, partner] + ([prev] if last else []) + list(consts)
    specs = [smem] * 3 + [vmem] * (len(operands) - 3)
    return pl.pallas_call(
        make_kernel(match_index, bit_pos, last),
        out_shape=jax.ShapeDtypeStruct(mine.shape, BF16),
        in_specs=specs,
        out_specs=vmem,
        scratch_shapes=[
            pltpu.VMEM((2 * EDGE + TILES, ROWS, LANES), F32),
            pltpu.VMEM((PAIRS * BOX, LANES), F32),
        ],
        compiler_params=pltpu.CompilerParams(vmem_limit_bytes=16 * 2**20),
        name="pair_last" if last else "pair_first",
    )(*operands)


def from_partner(block, axis, stride):
    count = lax.axis_size(axis)
    route = []
    for low in range(count):
        high = low | 1 << stride
        if high != low and high < count:
            route += [(low, high), (high, low)]
    return lax.ppermute(block, axis, route)


def per_device(orbitals, pair_mask, offsets):
    devices = lax.axis_size("orb")
    levels = devices.bit_length() - 1
    me = lax.axis_index("orb").astype(jnp.int32).reshape(1)
    matches = pair_mask.shape[0]
    consts = [jnp.asarray(t) for t in tables()]
    bits = [m * (levels - 1) // (matches - 1) for m in range(matches)]
    far = from_partner(orbitals, "orb", bits[1])
    near = from_partner(orbitals, "orb", bits[0])
    first = pair_call(0, bits[0], False, me, pair_mask, offsets, orbitals, near, None, consts)
    return pair_call(1, bits[1], True, me, pair_mask, offsets, orbitals, far, first, consts)


def solution(mesh):
    placed = (P("orb", None, None), P(), P())
    return jax.shard_map(
        per_device, mesh=mesh, in_specs=placed, out_specs=P("orb", None, None), check_vma=False
    )
```
